256 devices in a mesh: ens: 2 (over y_hi), time: 32 (over z, x), chan: 4 (over y_lo, core).
Axes of the slice: x: 4, y: 4 (y_hi: 2, y_lo: 2; y = y_hi * 2 + y_lo), z: 8, core: 2. Of those that a mesh axis runs over, the one named last changes fastest.
Arguments:
- decay_rate: float32 [4, 32768, 1024], P('ens', 'time', 'chan'), parts along dimension 0, may hold values from 0.2 to 2
- drive_in: bfloat16 [4, 32768, 1024], P('ens', 'time', 'chan'), parts along dimension 0, may hold values from -6 to 6
- gate_in: bfloat16 [4, 32768, 1024], P('ens', 'time', 'chan'), parts along dimension 0, may hold values from -6 to 6
- norm_gain: float32 [2048], P(('ens', 'chan')), parts along dimension 0, may hold values from 0.25 to 1.75
Outputs:
- mixed_out: bfloat16 [4, 32768, 1024], P('ens', 'time', 'chan'), parts along dimension 0
The draws below stay inside these ranges and needn't reach their ends.
There are 2 independent parts, one for each index of `ens`. The reference program is written for one: setup_inputs(seed, part) draws one part's arguments, and reference() takes and returns one part's arrays. A program takes and returns all parts, laid end to end along the dimension named above; each array names one. Nothing has to cross between parts.
All inputs are finite; a program needn't handle non-finite values.
Results may differ from the reference program's by a relative error of at most 0.001.
Values sent between devices are 32-bit elements.
No kernel may reach another device: no remote copies, remote signals or barrier semaphores. Data moves between devices by JAX's collectives and lax.ppermute only.
A program may use at most 64 MiB of HBM per device.

```python
import jax
import jax.numpy as jnp
from jax import lax

BATCH = 2
CHANNELS = 1024
LENGTH = 32768


def steps_of(stream_key, shape, pieces, least, high):
    level = 1.0
    for dim, parts in pieces:
        steps = jax.random.uniform(jax.random.fold_in(jax.random.fold_in(stream_key, 6), dim), (parts,), jnp.float32, least / len(pieces), high / len(pieces))
        level = level * jnp.repeat(jnp.exp(steps), shape[dim] // parts).reshape((-1,) + (1,) * (len(shape) - 1 - dim))
    return level


def scatter_about(key, dims, width, limit, shards=(), held_as=jnp.bfloat16):
    entries = width * jax.random.normal(key, dims, jnp.float32)
    if shards:
        entries = entries * steps_of(key, dims, shards, -0.22, 0.18)
    return jnp.clip(entries, -limit, limit).astype(held_as)


def setup_inputs(seed: int = 0, part: int = 0) -> dict:
    seeds = jax.random.split(jax.random.key(seed), 5)
    part_keys = jax.random.split(jax.random.fold_in(seeds[4], part), 5)
    return {
        "decay_rate": jnp.clip(0.2 + 1.8 * jax.random.uniform(part_keys[0], (BATCH, LENGTH, CHANNELS), jnp.float32) ** steps_of(part_keys[0], (BATCH, LENGTH, CHANNELS), ((1, 32), (2, 4)), -0.2, 0.2), 0.2, 2.0),
        "drive_in": scatter_about(part_keys[1], (BATCH, LENGTH, CHANNELS), 1.0, 6.0, ((1, 32), (2, 4))),
        "gate_in": scatter_about(part_keys[2], (BATCH, LENGTH, CHANNELS), 1.0, 6.0, ((1, 32), (2, 4))),
        "norm_gain": jnp.clip(1.0 + 0.15 * jax.random.normal(part_keys[3], (CHANNELS,), jnp.float32), 0.25, 1.75),
    }


def join_pair(earlier, later):
    return (earlier[0] * later[0], later[0] * earlier[1] + later[1])

def reference(decay_rate, drive_in, gate_in, norm_gain):
    keep = jnp.exp(-decay_rate / LENGTH)
    push = drive_in.astype(jnp.float32) * LENGTH ** (-0.5)
    forward = lax.associative_scan(join_pair, (keep, push), axis=1)[1]
    backward = lax.associative_scan(join_pair, (keep, push), axis=1, reverse=True)[1]
    states = forward + backward
    gated = states * jax.nn.silu(gate_in.astype(jnp.float32))
    power = lax.optimization_barrier(jnp.mean(gated * gated, axis=-1, keepdims=True))
    mixed_out = (gated * lax.rsqrt(power + 1e-06) * norm_gain).astype(jnp.bfloat16)
    return mixed_out
```

```python
import functools

import jax
import jax.numpy as jnp
from jax import lax
from jax.experimental import pallas as pl
from jax.experimental.pallas import tpu as pltpu
from jax.sharding import PartitionSpec as P

BLOCK = 128


def triangle(strict):
    row = lax.broadcasted_iota(jnp.int32, (BLOCK, 2 * BLOCK), 0)
    col = lax.broadcasted_iota(jnp.int32, (BLOCK, 2 * BLOCK), 1)
    col = jnp.where(col >= BLOCK, col - BLOCK, col)
    keep = col < row if strict else col <= row
    return jnp.where(keep, 1.0, 0.0).astype(jnp.bfloat16)


def stacked(top, bottom):
    return jnp.concatenate([top, bottom], axis=0)


def local_kernel(total_length, decay, drive, gate, gl, ga, gb, send,
                 decay_v, drive_v, gate_v, tile, sems):
    batch, length, chans = decay.shape
    blocks = length // BLOCK
    me = lax.axis_index("time")
    pairs = ((decay, decay_v), (drive, drive_v), (gate, gate_v))

    def copy(which, step):
        b, i = step // blocks, step % blocks
        src, dst = pairs[which]
        rows = pl.ds(i * BLOCK, BLOCK)
        return pltpu.make_async_copy(
            src.at[b, rows, :], dst.at[b, rows, :], sems.at[which, step])

    order = [b * blocks + i for i in range(blocks) for b in range(batch)]
    for step in order:
        for which in range(3):
            copy(which, step).start()
    upto = triangle(False)
    before = triangle(True)
    dot = functools.partial(jnp.dot, preferred_element_type=jnp.float32)
    carry = [[jnp.zeros((1, chans), jnp.float32)] * 3 for _ in range(batch)]
    for step in order:
        b, i = step // blocks, step % blocks
        for which in range(3):
            copy(which, step).wait()
        rows = pl.ds(i * BLOCK, BLOCK)
        sum_c, sum_f, sum_b = carry[b]
        d = decay_v[b, rows, :] * (1.0 / total_length)
        high = d.astype(jnp.bfloat16)
        low = (d - high.astype(jnp.float32)).astype(jnp.bfloat16)
        c = dot(upto, stacked(high, low)) + sum_c
        cp = c - d
        x16 = drive_v[b, rows, :]
        x = x16.astype(jnp.float32)
        v = ((jnp.exp(c) - 1.0) * x).astype(jnp.bfloat16)
        w = ((jnp.exp(-cp) - 1.0) * x).astype(jnp.bfloat16)
        f = dot(upto, stacked(x16, v)) + sum_f
        q = dot(before, stacked(x16, w)) + sum_b
        a = jnp.exp(-c)
        e = jnp.exp(cp)
        g = gate_v[b, rows, :].astype(jnp.float32)
        g = g / (1.0 + jnp.exp(-g))
        gl[b, rows, :] = g * (a * f - e * q)
        ga[b, rows, :] = g * a
        gb[b, rows, :] = g * e
        last = slice(BLOCK - 1, BLOCK)
        carry[b] = [
            c[last], f[last],
            q[last] + x[last] + w[last].astype(jnp.float32)]
    half = chans // 2
    for b in range(batch):
        sum_c, sum_f, sum_b = carry[b]
        p = jnp.exp(-sum_c)
        out_f = p * sum_f
        for k in range(2):
            cols = slice(k * half, (k + 1) * half)
            r = 2 * b + k
            for side, val in ((0, out_f), (1, sum_b)):
                tile[side, r:r + 1, :] = p[:, cols]
                tile[side, 4 + r:5 + r, :] = val[:, cols]
    rightward, leftward = tile[0], tile[1]
    for k in range(send.shape[0]):
        send[k] = jnp.where(k > me, rightward, leftward)


def states_kernel(recv, gl, ga, gb, gated, power):
    batch, length, chans = gl.shape
    devices = recv.shape[0]
    me = lax.axis_index("time")
    fwd = jnp.zeros(recv.shape[1:], jnp.float32)
    bwd = fwd
    for j in range(devices):
        got = recv[j]
        fwd = jnp.where(j < me, pltpu.roll(got, 4, 0) * fwd + got, fwd)
        j = devices - 1 - j
        got = recv[j]
        bwd = jnp.where(j >= me, pltpu.roll(got, 4, 0) * bwd + got, bwd)
    half = chans // 2
    for b in range(batch):
        for i in range(length // BLOCK):
            rows = pl.ds(i * BLOCK, BLOCK)
            total = None
            for k in range(2):
                cols = pl.ds(k * half, half)
                r = 4 + 2 * b + k
                s = (gl[b, rows, cols] + ga[b, rows, cols] * fwd[r:r + 1]
                     + gb[b, rows, cols] * bwd[r:r + 1])
                gated[b, rows, cols] = s
                total = s * s if k == 0 else total + s * s
            power[b, i:i + 1, :] = jnp.sum(total.T, axis=0, keepdims=True)


def scale_kernel(count, scale, gated, own, p1, p2, p3, gain, out):
    batch, length, chans = gated.shape
    half = chans // 2
    for b in range(batch):
        total = own[b] + p1[b] + p2[b] + p3[b]
        r = lax.rsqrt(total * (scale * scale / count) + 1e-06) * scale
        for i in range(length // BLOCK):
            rows = pl.ds(i * BLOCK, BLOCK)
            m = jnp.broadcast_to(r[i:i + 1, :], (BLOCK, BLOCK)).T
            for k in range(2):
                cols = pl.ds(k * half, half)
                out[b, rows, cols] = (
                    gated[b, rows, cols] * m * gain[:, cols]
                ).astype(jnp.bfloat16)


def on_device(decay_rate, drive_in, gate_in, norm_gain):
    batch, length, chans = decay_rate.shape
    devices = lax.axis_size("time")
    chan_devices = lax.axis_size("chan")
    total_length = length * devices
    steps = batch * (length // BLOCK)
    f32 = jnp.float32
    vmem = pl.BlockSpec(memory_space=pltpu.VMEM)
    hbm = pl.BlockSpec(memory_space=pltpu.HBM)
    full = jax.ShapeDtypeStruct((batch, length, chans), f32)
    gl, ga, gb, send = pl.pallas_call(
        functools.partial(local_kernel, total_length),
        out_shape=(full, full, full, jax.ShapeDtypeStruct((devices, 8, 128), f32)),
        in_specs=[hbm] * 3,
        out_specs=(vmem,) * 4,
        scratch_shapes=[
            pltpu.VMEM((batch, length, chans), f32),
            pltpu.VMEM((batch, length, chans), jnp.bfloat16),
            pltpu.VMEM((batch, length, chans), jnp.bfloat16),
            pltpu.VMEM((2, 8, 128), f32),
            pltpu.SemaphoreType.DMA((3, steps)),
        ],
        compiler_params=pltpu.CompilerParams(vmem_limit_bytes=32 << 20),
        name="local",
    )(*(pltpu.with_memory_space_constraint(a, pltpu.HBM)
        for a in (decay_rate, drive_in, gate_in)))
    recv = lax.all_to_all(send, "time", 0, 0)
    gated, power = pl.pallas_call(
        states_kernel,
        out_shape=(full, jax.ShapeDtypeStruct((batch, length // BLOCK, BLOCK), f32)),
        in_specs=[vmem] * 4,
        out_specs=(vmem,) * 2,
        compiler_params=pltpu.CompilerParams(vmem_limit_bytes=32 << 20),
        name="states",
    )(recv, gl, ga, gb)
    others = [
        lax.ppermute(power, "chan", [(i, i ^ k) for i in range(chan_devices)])
        for k in range(1, chan_devices)
    ]
    return pl.pallas_call(
        functools.partial(scale_kernel, chans * chan_devices, float(total_length) ** -0.5),
        out_shape=jax.ShapeDtypeStruct((batch, length, chans), jnp.bfloat16),
        in_specs=[vmem] * 6,
        out_specs=vmem,
        compiler_params=pltpu.CompilerParams(vmem_limit_bytes=32 << 20),
        name="scale",
    )(gated, power, *others, norm_gain.reshape(1, chans))


def solution(mesh):
    spec = P("ens", "time", "chan")
    return jax.shard_map(
        on_device, mesh=mesh, in_specs=(spec, spec, spec, P(("ens", "chan"))),
        out_specs=spec, check_vma=False,
    )
```

```python
import functools

import jax
import jax.numpy as jnp
from jax import lax
from jax.experimental import pallas as pl
from jax.experimental.pallas import tpu as pltpu
from jax.sharding import PartitionSpec as P

BLOCK = 128
LOG2E = 1.4426950408889634


def triangle(strict):
    row = lax.broadcasted_iota(jnp.int32, (BLOCK, 2 * BLOCK), 0)
    col = lax.broadcasted_iota(jnp.int32, (BLOCK, 2 * BLOCK), 1)
    col = jnp.where(col >= BLOCK, col - BLOCK, col)
    keep = col < row if strict else col <= row
    return jnp.where(keep, 1.0, 0.0).astype(jnp.bfloat16)


def stacked(top, bottom):
    return jnp.concatenate([top, bottom], axis=0)


def local_kernel(total_length, decay, drive, a_out, e_out, f_out, q_out, ends, send,
                 decay_v, drive_v, c_v, v_v, w_v, tile, sems):
    batch, length, chans = decay.shape
    blocks = length // BLOCK
    me = lax.axis_index("time")
    unit = LOG2E / total_length
    pairs = ((decay, decay_v), (drive, drive_v))

    def copy(which, b, i):
        src, dst = pairs[which]
        rows = pl.ds(i * BLOCK, BLOCK)
        return pltpu.make_async_copy(
            src.at[b, rows, :], dst.at[b, rows, :], sems.at[which, b, i])

    for i in range(blocks):
        for b in range(batch):
            for which in range(2):
                copy(which, b, i).start()
    upto = triangle(False)
    before = triangle(True)
    dot = functools.partial(jnp.dot, preferred_element_type=jnp.float32)
    last = slice(BLOCK - 1, BLOCK)

    def prefix(b, i):
        rows = pl.ds(i * BLOCK, BLOCK)
        n = decay_v[b, rows, :] * -unit
        high = n.astype(jnp.bfloat16)
        low = (n - high.astype(jnp.float32)).astype(jnp.bfloat16)
        c_v[b, rows, :] = dot(upto, stacked(high, low))

    def weights(b, i):
        rows = pl.ds(i * BLOCK, BLOCK)
        d = decay_v[b, rows, :]
        c = c_v[b, rows, :]
        a = jnp.exp2(c)
        e = jnp.exp2(d * -unit - c)
        step = jnp.exp2(d * unit)
        a_out[b, rows, :] = a
        e_out[b, rows, :] = e
        x = drive_v[b, rows, :].astype(jnp.float32)
        v_v[b, rows, :] = ((e * step - 1.0) * x).astype(jnp.bfloat16)
        w_v[b, rows, :] = ((a * step - 1.0) * x).astype(jnp.bfloat16)
        ends[0, b, pl.ds(i, 1), :] = a[last]

    def sums(b, i):
        rows = pl.ds(i * BLOCK, BLOCK)
        x = drive_v[b, rows, :]
        w = w_v[b, rows, :]
        f = dot(upto, stacked(x, v_v[b, rows, :]))
        q = dot(before, stacked(x, w))
        f_out[b, rows, :] = f
        q_out[b, rows, :] = q
        ends[1, b, pl.ds(i, 1), :] = f[last]
        ends[2, b, pl.ds(i, 1), :] = (
            q[last] + x[last].astype(jnp.float32) + w[last].astype(jnp.float32))

    for s in range(blocks + 2):
        if s < blocks:
            for b in range(batch):
                for which in range(2):
                    copy(which, b, s).wait()
        for b in range(batch):
            if s >= 2:
                sums(b, s - 2)
            if 1 <= s <= blocks:
                weights(b, s - 1)
            if s < blocks:
                prefix(b, s)
    half = chans // 2
    for b in range(batch):
        fwd = bwd = jnp.zeros((1, chans), jnp.float32)
        p = jnp.ones((1, chans), jnp.float32)
        for i in range(blocks):
            j = blocks - 1 - i
            fwd = ends[0, b, i:i + 1, :] * (fwd + ends[1, b, i:i + 1, :])
            bwd = ends[2, b, j:j + 1, :] + ends[0, b, j:j + 1, :] * bwd
            p = p * ends[0, b, i:i + 1, :]
        for k in range(2):
            cols = slice(k * half, (k + 1) * half)
            r = 2 * b + k
            for side, val in ((0, fwd), (1, bwd)):
                tile[side, r:r + 1, :] = p[:, cols]
                tile[side, 4 + r:5 + r, :] = val[:, cols]
    rightward, leftward = tile[0], tile[1]
    for k in range(send.shape[0]):
        send[k] = jnp.where(k > me, rightward, leftward)


def states_kernel(recv, ends, a, e, f, q, gate, gated, power):
    batch, length, chans = a.shape
    blocks = length // BLOCK
    devices = recv.shape[0]
    me = lax.axis_index("time")
    fwd = jnp.zeros(recv.shape[1:], jnp.float32)
    bwd = fwd
    for j in range(devices):
        got = recv[j]
        fwd = jnp.where(j < me, pltpu.roll(got, 4, 0) * fwd + got, fwd)
        j = devices - 1 - j
        got = recv[j]
        bwd = jnp.where(j > me, pltpu.roll(got, 4, 0) * bwd + got, bwd)
    half = chans // 2
    for b in range(batch):
        alpha = [[None] * blocks for _ in range(2)]
        beta = [[None] * blocks for _ in range(2)]
        for k in range(2):
            cols = pl.ds(k * half, half)
            r = 4 + 2 * b + k
            state = fwd[r:r + 1]
            for i in range(blocks):
                alpha[k][i] = state
                state = ends[0, b, i:i + 1, cols] * (state + ends[1, b, i:i + 1, cols])
            state = bwd[r:r + 1]
            for i in reversed(range(blocks)):
                state = ends[2, b, i:i + 1, cols] + ends[0, b, i:i + 1, cols] * state
                beta[k][i] = state
        for i in range(blocks):
            rows = pl.ds(i * BLOCK, BLOCK)
            total = None
            for k in range(2):
                cols = pl.ds(k * half, half)
                h = gate[b, rows, cols].astype(jnp.float32) * 0.5
                s = (h + h * jnp.tanh(h)) * (
                    a[b, rows, cols] * (f[b, rows, cols] + alpha[k][i])
                    + e[b, rows, cols] * (beta[k][i] - q[b, rows, cols]))
                gated[b, rows, cols] = s
                total = s * s if k == 0 else total + s * s
            power[b, i:i + 1, :] = jnp.sum(total.T, axis=0, keepdims=True)


def scale_kernel(count, scale, gated, own, p1, p2, p3, gain, out, stage, sems):
    batch, length, chans = gated.shape
    half = chans // 2
    copies = []
    for b in range(batch):
        total = own[b] + p1[b] + p2[b] + p3[b]
        r = lax.rsqrt(total * (scale * scale / count) + 1e-06) * scale
        for i in range(length // BLOCK):
            rows = pl.ds(i * BLOCK, BLOCK)
            m = jnp.broadcast_to(r[i:i + 1, :], (BLOCK, BLOCK)).T
            for k in range(2):
                cols = pl.ds(k * half, half)
                stage[b, rows, cols] = (
                    gated[b, rows, cols] * m * gain[:, cols]
                ).astype(jnp.bfloat16)
            copies.append(pltpu.make_async_copy(
                stage.at[b, rows, :], out.at[b, rows, :], sems.at[b, i]))
            copies[-1].start()
    for c in copies:
        c.wait()


def on_device(decay_rate, drive_in, gate_in, norm_gain):
    batch, length, chans = decay_rate.shape
    blocks = length // BLOCK
    devices = lax.axis_size("time")
    chan_devices = lax.axis_size("chan")
    total_length = length * devices
    f32 = jnp.float32
    vmem = pl.BlockSpec(memory_space=pltpu.VMEM)
    hbm = pl.BlockSpec(memory_space=pltpu.HBM)
    full = jax.ShapeDtypeStruct((batch, length, chans), f32)
    a, e, f, q, ends, send = pl.pallas_call(
        functools.partial(local_kernel, total_length),
        out_shape=(full,) * 4 + (
            jax.ShapeDtypeStruct((3, batch, blocks, chans), f32),
            jax.ShapeDtypeStruct((devices, 8, 128), f32)),
        in_specs=[hbm] * 2,
        out_specs=(vmem,) * 6,
        scratch_shapes=[
            pltpu.VMEM((batch, length, chans), f32),
            pltpu.VMEM((batch, length, chans), jnp.bfloat16),
            pltpu.VMEM((batch, length, chans), f32),
            pltpu.VMEM((batch, length, chans), jnp.bfloat16),
            pltpu.VMEM((batch, length, chans), jnp.bfloat16),
            pltpu.VMEM((2, 8, 128), f32),
            pltpu.SemaphoreType.DMA((2, batch, blocks)),
        ],
        compiler_params=pltpu.CompilerParams(vmem_limit_bytes=32 << 20),
        name="local",
    )(*(pltpu.with_memory_space_constraint(t, pltpu.HBM)
        for t in (decay_rate, drive_in)))
    recv = lax.all_to_all(send, "time", 0, 0)
    gated, power = pl.pallas_call(
        states_kernel,
        out_shape=(full, jax.ShapeDtypeStruct((batch, blocks, BLOCK), f32)),
        in_specs=[vmem] * 7,
        out_specs=(vmem,) * 2,
        compiler_params=pltpu.CompilerParams(vmem_limit_bytes=32 << 20),
        name="states",
    )(recv, ends, a, e, f, q, gate_in)
    others = [
        lax.ppermute(power, "chan", [(i, i ^ k) for i in range(chan_devices)])
        for k in range(1, chan_devices)
    ]
    return pl.pallas_call(
        functools.partial(scale_kernel, chans * chan_devices, float(total_length) ** -0.5),
        out_shape=jax.ShapeDtypeStruct((batch, length, chans), jnp.bfloat16),
        in_specs=[vmem] * 6,
        out_specs=hbm,
        scratch_shapes=[
            pltpu.VMEM((batch, length, chans), jnp.bfloat16),
            pltpu.SemaphoreType.DMA((batch, blocks)),
        ],
        compiler_params=pltpu.CompilerParams(vmem_limit_bytes=32 << 20),
        name="scale",
    )(gated, power, *others, norm_gain.reshape(1, chans))


def solution(mesh):
    spec = P("ens", "time", "chan")
    return jax.shard_map(
        on_device, mesh=mesh, in_specs=(spec, spec, spec, P(("ens", "chan"))),
        out_specs=spec, check_vma=False,
    )
```

```python
import functools

import jax
import jax.numpy as jnp
from jax import lax
from jax.experimental import pallas as pl
from jax.experimental.pallas import tpu as pltpu
from jax.sharding import PartitionSpec as P

BLOCK = 128
TILE = 16
WAITS = (0, 1, 4)
LOG2E = 1.4426950408889634


def triangle(strict):
    row = lax.broadcasted_iota(jnp.int32, (BLOCK, 2 * BLOCK), 0)
    col = lax.broadcasted_iota(jnp.int32, (BLOCK, 2 * BLOCK), 1)
    col = jnp.where(col >= BLOCK, col - BLOCK, col)
    keep = col < row if strict else col <= row
    return jnp.where(keep, 1.0, 0.0).astype(jnp.bfloat16)


def stacked(top, bottom):
    return jnp.concatenate([top, bottom], axis=0)


def local_kernel(total_length, decay, drive, a_out, e_out, f_out, q_out, ends, send,
                 decay_v, drive_v, n_v, c_v, v_v, w_v, tile, sems):
    batch, length, chans = decay.shape
    blocks = length // BLOCK
    me = lax.axis_index("time")
    unit = LOG2E / total_length
    pairs = ((decay, decay_v), (drive, drive_v))

    def copy(which, b, i):
        src, dst = pairs[which]
        rows = pl.ds(i * BLOCK, BLOCK)
        return pltpu.make_async_copy(
            src.at[b, rows, :], dst.at[b, rows, :], sems.at[which, b, i])

    for i in range(blocks):
        for b in range(batch):
            for which in range(2):
                copy(which, b, i).start()
    upto = triangle(False)
    before = triangle(True)
    dot = functools.partial(jnp.dot, preferred_element_type=jnp.float32)
    last = slice(BLOCK - 1, BLOCK)

    def split(b, i):
        for r in range(0, BLOCK, TILE):
            n = decay_v[b, pl.ds(i * BLOCK + r, TILE), :] * -unit
            high = n.astype(jnp.bfloat16)
            low = (n - high.astype(jnp.float32)).astype(jnp.bfloat16)
            n_v[b, i, pl.ds(r, TILE), :] = high
            n_v[b, i, pl.ds(BLOCK + r, TILE), :] = low

    def prefix(b, i):
        c_v[b, pl.ds(i * BLOCK, BLOCK), :] = dot(upto, n_v[b, i])

    def weights(b, i):
        for r in range(0, BLOCK, TILE):
            rows = pl.ds(i * BLOCK + r, TILE)
            d = decay_v[b, rows, :]
            c = c_v[b, rows, :]
            a = jnp.exp2(c)
            e = jnp.exp2(d * -unit - c)
            step = jnp.exp2(d * unit)
            a_out[b, rows, :] = a
            e_out[b, rows, :] = e
            x = drive_v[b, rows, :].astype(jnp.float32)
            v_v[b, rows, :] = ((e * step - 1.0) * x).astype(jnp.bfloat16)
            w_v[b, rows, :] = ((a * step - 1.0) * x).astype(jnp.bfloat16)
        ends[0, b, pl.ds(i, 1), :] = a[TILE - 1:TILE]

    def sums(b, i):
        rows = pl.ds(i * BLOCK, BLOCK)
        x = drive_v[b, rows, :]
        w = w_v[b, rows, :]
        f = dot(upto, stacked(x, v_v[b, rows, :]))
        q = dot(before, stacked(x, w))
        f_out[b, rows, :] = f
        q_out[b, rows, :] = q
        ends[1, b, pl.ds(i, 1), :] = f[last]
        ends[2, b, pl.ds(i, 1), :] = (
            q[last] + x[last].astype(jnp.float32) + w[last].astype(jnp.float32))

    waits = {at: stop for at, stop in zip(WAITS, WAITS[1:] + (blocks,))}
    for s in range(blocks + 3):
        if s in waits:
            for i in range(s, waits[s]):
                for b in range(batch):
                    for which in range(2):
                        copy(which, b, i).wait()
        for b in range(batch):
            if s >= 3:
                sums(b, s - 3)
            if 1 <= s <= blocks:
                prefix(b, s - 1)
        for b in range(batch):
            if 2 <= s <= blocks + 1:
                weights(b, s - 2)
            if s < blocks:
                split(b, s)
    half = chans // 2
    for b in range(batch):
        fwd = bwd = jnp.zeros((1, chans), jnp.float32)
        p = jnp.ones((1, chans), jnp.float32)
        for i in range(blocks):
            j = blocks - 1 - i
            fwd = ends[0, b, i:i + 1, :] * (fwd + ends[1, b, i:i + 1, :])
            bwd = ends[2, b, j:j + 1, :] + ends[0, b, j:j + 1, :] * bwd
            p = p * ends[0, b, i:i + 1, :]
        for k in range(2):
            cols = slice(k * half, (k + 1) * half)
            r = 2 * b + k
            for side, val in ((0, fwd), (1, bwd)):
                tile[side, r:r + 1, :] = p[:, cols]
                tile[side, 4 + r:5 + r, :] = val[:, cols]
    rightward, leftward = tile[0], tile[1]
    for k in range(send.shape[0]):
        send[k] = jnp.where(k > me, rightward, leftward)


def states_kernel(recv, ends, a, e, f, q, gate, gated, power):
    batch, length, chans = a.shape
    blocks = length // BLOCK
    devices = recv.shape[0]
    me = lax.axis_index("time")
    fwd = jnp.zeros(recv.shape[1:], jnp.float32)
    bwd = fwd
    for j in range(devices):
        got = recv[j]
        fwd = jnp.where(j < me, pltpu.roll(got, 4, 0) * fwd + got, fwd)
        j = devices - 1 - j
        got = recv[j]
        bwd = jnp.where(j > me, pltpu.roll(got, 4, 0) * bwd + got, bwd)
    half = chans // 2
    for b in range(batch):
        alpha = [[None] * blocks for _ in range(2)]
        beta = [[None] * blocks for _ in range(2)]
        for k in range(2):
            cols = pl.ds(k * half, half)
            r = 4 + 2 * b + k
            state = fwd[r:r + 1]
            for i in range(blocks):
                alpha[k][i] = state
                state = ends[0, b, i:i + 1, cols] * (state + ends[1, b, i:i + 1, cols])
            state = bwd[r:r + 1]
            for i in reversed(range(blocks)):
                state = ends[2, b, i:i + 1, cols] + ends[0, b, i:i + 1, cols] * state
                beta[k][i] = state
        for i in range(blocks):
            rows = pl.ds(i * BLOCK, BLOCK)
            total = None
            for k in range(2):
                cols = pl.ds(k * half, half)
                h = gate[b, rows, cols].astype(jnp.float32) * 0.5
                s = (h + h * jnp.tanh(h)) * (
                    a[b, rows, cols] * (f[b, rows, cols] + alpha[k][i])
                    + e[b, rows, cols] * (beta[k][i] - q[b, rows, cols]))
                gated[b, rows, cols] = s
                total = s * s if k == 0 else total + s * s
            power[b, i:i + 1, :] = jnp.sum(total.T, axis=0, keepdims=True)


def scale_kernel(count, scale, gated, own, p1, p2, p3, gain, out, stage, sems):
    batch, length, chans = gated.shape
    half = chans // 2
    copies = []
    for b in range(batch):
        total = own[b] + p1[b] + p2[b] + p3[b]
        r = lax.rsqrt(total * (scale * scale / count) + 1e-06) * scale
        for i in range(length // BLOCK):
            rows = pl.ds(i * BLOCK, BLOCK)
            m = jnp.broadcast_to(r[i:i + 1, :], (BLOCK, BLOCK)).T
            for k in range(2):
                cols = pl.ds(k * half, half)
                stage[b, rows, cols] = (
                    gated[b, rows, cols] * m * gain[:, cols]
                ).astype(jnp.bfloat16)
            copies.append(pltpu.make_async_copy(
                stage.at[b, rows, :], out.at[b, rows, :], sems.at[b, i]))
            copies[-1].start()
    for c in copies:
        c.wait()


def on_device(decay_rate, drive_in, gate_in, norm_gain):
    batch, length, chans = decay_rate.shape
    blocks = length // BLOCK
    devices = lax.axis_size("time")
    chan_devices = lax.axis_size("chan")
    total_length = length * devices
    f32 = jnp.float32
    vmem = pl.BlockSpec(memory_space=pltpu.VMEM)
    hbm = pl.BlockSpec(memory_space=pltpu.HBM)
    full = jax.ShapeDtypeStruct((batch, length, chans), f32)
    a, e, f, q, ends, send = pl.pallas_call(
        functools.partial(local_kernel, total_length),
        out_shape=(full,) * 4 + (
            jax.ShapeDtypeStruct((3, batch, blocks, chans), f32),
            jax.ShapeDtypeStruct((devices, 8, 128), f32)),
        in_specs=[hbm] * 2,
        out_specs=(vmem,) * 6,
        scratch_shapes=[
            pltpu.VMEM((batch, length, chans), f32),
            pltpu.VMEM((batch, length, chans), jnp.bfloat16),
            pltpu.VMEM((batch, blocks, 2 * BLOCK, chans), jnp.bfloat16),
            pltpu.VMEM((batch, length, chans), f32),
            pltpu.VMEM((batch, length, chans), jnp.bfloat16),
            pltpu.VMEM((batch, length, chans), jnp.bfloat16),
            pltpu.VMEM((2, 8, 128), f32),
            pltpu.SemaphoreType.DMA((2, batch, blocks)),
        ],
        compiler_params=pltpu.CompilerParams(vmem_limit_bytes=32 << 20),
        name="local",
    )(*(pltpu.with_memory_space_constraint(t, pltpu.HBM)
        for t in (decay_rate, drive_in)))
    recv = lax.all_to_all(send, "time", 0, 0)
    gated, power = pl.pallas_call(
        states_kernel,
        out_shape=(full, jax.ShapeDtypeStruct((batch, blocks, BLOCK), f32)),
        in_specs=[vmem] * 7,
        out_specs=(vmem,) * 2,
        compiler_params=pltpu.CompilerParams(vmem_limit_bytes=32 << 20),
        name="states",
    )(recv, ends, a, e, f, q, gate_in)
    others = [
        lax.ppermute(power, "chan", [(i, i ^ k) for i in range(chan_devices)])
        for k in range(1, chan_devices)
    ]
    return pl.pallas_call(
        functools.partial(scale_kernel, chans * chan_devices, float(total_length) ** -0.5),
        out_shape=jax.ShapeDtypeStruct((batch, length, chans), jnp.bfloat16),
        in_specs=[vmem] * 6,
        out_specs=hbm,
        scratch_shapes=[
            pltpu.VMEM((batch, length, chans), jnp.bfloat16),
            pltpu.SemaphoreType.DMA((batch, blocks)),
        ],
        compiler_params=pltpu.CompilerParams(vmem_limit_bytes=32 << 20),
        name="scale",
    )(gated, power, *others, norm_gain.reshape(1, chans))


def solution(mesh):
    spec = P("ens", "time", "chan")
    return jax.shard_map(
        on_device, mesh=mesh, in_specs=(spec, spec, spec, P(("ens", "chan"))),
        out_specs=spec, check_vma=False,
    )
```

```python
import functools

import jax
import jax.numpy as jnp
from jax import lax
from jax.experimental import pallas as pl
from jax.experimental.pallas import tpu as pltpu
from jax.sharding import PartitionSpec as P

BLOCK = 128
TILE = 16
WAITS = (0, 1, 3, 5)
LOG2E = 1.4426950408889634


def triangle(strict):
    row = lax.broadcasted_iota(jnp.int32, (BLOCK, 2 * BLOCK), 0)
    col = lax.broadcasted_iota(jnp.int32, (BLOCK, 2 * BLOCK), 1)
    col = jnp.where(col >= BLOCK, col - BLOCK, col)
    keep = col < row if strict else col <= row
    return jnp.where(keep, 1.0, 0.0).astype(jnp.bfloat16)


def stacked(top, bottom):
    return jnp.concatenate([top, bottom], axis=0)


def local_kernel(total_length, decay, drive, a_out, e_out, f_out, q_out, ends, send,
                 decay_v, drive_v, n_v, c_v, v_v, w_v, tile, sems):
    batch, length, chans = decay.shape
    blocks = length // BLOCK
    me = lax.axis_index("time")
    unit = LOG2E / total_length
    pairs = ((decay, decay_v), (drive, drive_v))

    waits = {at: stop for at, stop in zip(WAITS, WAITS[1:] + (blocks,))}

    def copy(which, i):
        src, dst = pairs[which]
        rows = pl.ds(i * BLOCK, (waits[i] - i) * BLOCK)
        return pltpu.make_async_copy(
            src.at[:, rows, :], dst.at[:, rows, :], sems.at[which, i])

    for i in WAITS:
        for which in range(2):
            copy(which, i).start()
    upto = triangle(False)
    before = triangle(True)
    dot = functools.partial(jnp.dot, preferred_element_type=jnp.float32)
    last = slice(BLOCK - 1, BLOCK)

    def split(b, i):
        for r in range(0, BLOCK, TILE):
            n = decay_v[b, pl.ds(i * BLOCK + r, TILE), :] * -unit
            high = n.astype(jnp.bfloat16)
            low = (n - high.astype(jnp.float32)).astype(jnp.bfloat16)
            n_v[b, i, pl.ds(r, TILE), :] = high
            n_v[b, i, pl.ds(BLOCK + r, TILE), :] = low

    def prefix(b, i):
        c_v[b, pl.ds(i * BLOCK, BLOCK), :] = dot(upto, n_v[b, i])

    def weights(b, i):
        for r in range(0, BLOCK, TILE):
            rows = pl.ds(i * BLOCK + r, TILE)
            d = decay_v[b, rows, :]
            c = c_v[b, rows, :]
            a = jnp.exp2(c)
            e = jnp.exp2(d * -unit - c)
            step = jnp.exp2(d * unit)
            a_out[b, rows, :] = a
            e_out[b, rows, :] = e
            x = drive_v[b, rows, :].astype(jnp.float32)
            grown = x * step
            v_v[b, rows, :] = (e * grown - x).astype(jnp.bfloat16)
            w_v[b, rows, :] = (a * grown - x).astype(jnp.bfloat16)
        ends[0, b, pl.ds(i, 1), :] = a[TILE - 1:TILE]

    def sums(b, i):
        rows = pl.ds(i * BLOCK, BLOCK)
        x = drive_v[b, rows, :]
        w = w_v[b, rows, :]
        f = dot(upto, stacked(x, v_v[b, rows, :]))
        q = dot(before, stacked(x, w))
        f_out[b, rows, :] = f
        q_out[b, rows, :] = q
        ends[1, b, pl.ds(i, 1), :] = f[last]
        ends[2, b, pl.ds(i, 1), :] = (
            q[last] + x[last].astype(jnp.float32) + w[last].astype(jnp.float32))

    for s in range(blocks + 3):
        if s in waits:
            for which in range(2):
                copy(which, s).wait()
        for b in range(batch):
            if s >= 3:
                sums(b, s - 3)
            if 1 <= s <= blocks:
                prefix(b, s - 1)
        for b in range(batch):
            if 2 <= s <= blocks + 1:
                weights(b, s - 2)
            if s < blocks:
                split(b, s)
    half = chans // 2
    for b in range(batch):
        fwd = bwd = jnp.zeros((1, chans), jnp.float32)
        p = jnp.ones((1, chans), jnp.float32)
        for i in range(blocks):
            j = blocks - 1 - i
            fwd = ends[0, b, i:i + 1, :] * (fwd + ends[1, b, i:i + 1, :])
            bwd = ends[2, b, j:j + 1, :] + ends[0, b, j:j + 1, :] * bwd
            p = p * ends[0, b, i:i + 1, :]
        for k in range(2):
            cols = slice(k * half, (k + 1) * half)
            r = 2 * b + k
            for side, val in ((0, fwd), (1, bwd)):
                tile[side, r:r + 1, :] = p[:, cols]
                tile[side, 4 + r:5 + r, :] = val[:, cols]
    rightward, leftward = tile[0], tile[1]
    for k in range(send.shape[0]):
        send[k] = jnp.where(k > me, rightward, leftward)


def states_kernel(recv, ends, a, e, f, q, gate, gated, power):
    batch, length, chans = a.shape
    blocks = length // BLOCK
    devices = recv.shape[0]
    me = lax.axis_index("time")
    fwd = jnp.zeros(recv.shape[1:], jnp.float32)
    bwd = fwd
    for j in range(devices):
        got = recv[j]
        fwd = (jnp.where(j < me, pltpu.roll(got, 4, 0), 1.0) * fwd
               + jnp.where(j < me, got, 0.0))
        j = devices - 1 - j
        got = recv[j]
        bwd = (jnp.where(j > me, pltpu.roll(got, 4, 0), 1.0) * bwd
               + jnp.where(j > me, got, 0.0))
    half = chans // 2
    for b in range(batch):
        alpha = [[None] * blocks for _ in range(2)]
        beta = [[None] * blocks for _ in range(2)]
        for k in range(2):
            cols = pl.ds(k * half, half)
            r = 4 + 2 * b + k
            state = fwd[r:r + 1]
            for i in range(blocks):
                alpha[k][i] = state
                state = ends[0, b, i:i + 1, cols] * (state + ends[1, b, i:i + 1, cols])
            state = bwd[r:r + 1]
            for i in reversed(range(blocks)):
                state = ends[2, b, i:i + 1, cols] + ends[0, b, i:i + 1, cols] * state
                beta[k][i] = state
        for i in range(blocks):
            rows = pl.ds(i * BLOCK, BLOCK)
            total = None
            for k in range(2):
                cols = pl.ds(k * half, half)
                h = (gate[b, rows, cols] * 0.5).astype(jnp.float32)
                s = (h + h * jnp.tanh(h)) * (
                    a[b, rows, cols] * (f[b, rows, cols] + alpha[k][i])
                    + e[b, rows, cols] * (beta[k][i] - q[b, rows, cols]))
                gated[b, rows, cols] = s
                total = s * s if k == 0 else total + s * s
            power[b, i:i + 1, :] = jnp.sum(total.T, axis=0, keepdims=True)


def scale_kernel(count, scale, gated, own, p1, p2, p3, gain, out, stage, sems):
    batch, length, chans = gated.shape
    half = chans // 2
    copies = []
    for b in range(batch):
        total = own[b] + p1[b] + p2[b] + p3[b]
        r = lax.rsqrt(total * (scale * scale / count) + 1e-06) * scale
        for i in range(length // BLOCK):
            rows = pl.ds(i * BLOCK, BLOCK)
            m = jnp.broadcast_to(r[i:i + 1, :], (BLOCK, BLOCK)).T
            for k in range(2):
                cols = pl.ds(k * half, half)
                stage[b, rows, cols] = (
                    gated[b, rows, cols] * m * gain[:, cols]
                ).astype(jnp.bfloat16)
            copies.append(pltpu.make_async_copy(
                stage.at[b, rows, :], out.at[b, rows, :], sems.at[b, i]))
            copies[-1].start()
    for c in copies:
        c.wait()


def on_device(decay_rate, drive_in, gate_in, norm_gain):
    batch, length, chans = decay_rate.shape
    blocks = length // BLOCK
    devices = lax.axis_size("time")
    chan_devices = lax.axis_size("chan")
    total_length = length * devices
    f32 = jnp.float32
    vmem = pl.BlockSpec(memory_space=pltpu.VMEM)
    hbm = pl.BlockSpec(memory_space=pltpu.HBM)
    full = jax.ShapeDtypeStruct((batch, length, chans), f32)
    a, e, f, q, ends, send = pl.pallas_call(
        functools.partial(local_kernel, total_length),
        out_shape=(full,) * 4 + (
            jax.ShapeDtypeStruct((3, batch, blocks, chans), f32),
            jax.ShapeDtypeStruct((devices, 8, 128), f32)),
        in_specs=[hbm] * 2,
        out_specs=(vmem,) * 6,
        scratch_shapes=[
            pltpu.VMEM((batch, length, chans), f32),
            pltpu.VMEM((batch, length, chans), jnp.bfloat16),
            pltpu.VMEM((batch, blocks, 2 * BLOCK, chans), jnp.bfloat16),
            pltpu.VMEM((batch, length, chans), f32),
            pltpu.VMEM((batch, length, chans), jnp.bfloat16),
            pltpu.VMEM((batch, length, chans), jnp.bfloat16),
            pltpu.VMEM((2, 8, 128), f32),
            pltpu.SemaphoreType.DMA((2, blocks)),
        ],
        compiler_params=pltpu.CompilerParams(vmem_limit_bytes=32 << 20),
        name="local",
    )(*(pltpu.with_memory_space_constraint(t, pltpu.HBM)
        for t in (decay_rate, drive_in)))
    recv = lax.all_to_all(send, "time", 0, 0)
    gated, power = pl.pallas_call(
        states_kernel,
        out_shape=(full, jax.ShapeDtypeStruct((batch, blocks, BLOCK), f32)),
        in_specs=[vmem] * 7,
        out_specs=(vmem,) * 2,
        compiler_params=pltpu.CompilerParams(vmem_limit_bytes=32 << 20),
        name="states",
    )(recv, ends, a, e, f, q, gate_in)
    others = [
        lax.ppermute(power, "chan", [(i, i ^ k) for i in range(chan_devices)])
        for k in range(1, chan_devices)
    ]
    return pl.pallas_call(
        functools.partial(scale_kernel, chans * chan_devices, float(total_length) ** -0.5),
        out_shape=jax.ShapeDtypeStruct((batch, length, chans), jnp.bfloat16),
        in_specs=[vmem] * 6,
        out_specs=hbm,
        scratch_shapes=[
            pltpu.VMEM((batch, length, chans), jnp.bfloat16),
            pltpu.SemaphoreType.DMA((batch, blocks)),
        ],
        compiler_params=pltpu.CompilerParams(vmem_limit_bytes=32 << 20),
        name="scale",
    )(gated, power, *others, norm_gain.reshape(1, chans))


def solution(mesh):
    spec = P("ens", "time", "chan")
    return jax.shard_map(
        on_device, mesh=mesh, in_specs=(spec, spec, spec, P(("ens", "chan"))),
        out_specs=spec, check_vma=False,
    )
```

```python
import functools

import jax
import jax.numpy as jnp
from jax import lax
from jax.experimental import pallas as pl
from jax.experimental.pallas import tpu as pltpu
from jax.sharding import PartitionSpec as P

BLOCK = 128
TILE = 16
WAITS = (0, 1, 3, 5)
OUT = (0, 1, 2, 3, 4, 5, 6, 7)
LOG2E = 1.4426950408889634


def triangle(strict):
    row = lax.broadcasted_iota(jnp.int32, (BLOCK, 2 * BLOCK), 0)
    col = lax.broadcasted_iota(jnp.int32, (BLOCK, 2 * BLOCK), 1)
    col = jnp.where(col >= BLOCK, col - BLOCK, col)
    keep = col < row if strict else col <= row
    return jnp.where(keep, 1.0, 0.0).astype(jnp.bfloat16)


def stacked(top, bottom):
    return jnp.concatenate([top, bottom], axis=0)


def local_kernel(total_length, decay, drive, a_out, e_out, f_out, q_out, ends, send,
                 decay_v, drive_v, n_v, c_v, v_v, w_v, tile, sems):
    batch, length, chans = decay.shape
    blocks = length // BLOCK
    me = lax.axis_index("time")
    unit = LOG2E / total_length
    pairs = ((decay, decay_v), (drive, drive_v))

    waits = {at: stop for at, stop in zip(WAITS, WAITS[1:] + (blocks,))}

    def copy(which, i):
        src, dst = pairs[which]
        rows = pl.ds(i * BLOCK, (waits[i] - i) * BLOCK)
        return pltpu.make_async_copy(
            src.at[:, rows, :], dst.at[:, rows, :], sems.at[which, i])

    for i in WAITS:
        for which in range(2):
            copy(which, i).start()
    upto = triangle(False)
    before = triangle(True)
    dot = functools.partial(jnp.dot, preferred_element_type=jnp.float32)
    last = slice(BLOCK - 1, BLOCK)

    def split(b, i):
        for r in range(0, BLOCK, TILE):
            n = decay_v[b, pl.ds(i * BLOCK + r, TILE), :] * -unit
            n_v[b, i, pl.ds(r, TILE), :] = n.astype(jnp.bfloat16)
            part = n if r == 0 else part + n
        ends[0, b, pl.ds(i, 1), :] = jnp.exp2(jnp.sum(part, axis=0, keepdims=True))

    def prefix(b, i):
        c_v[b, pl.ds(i * BLOCK, BLOCK), :] = dot(upto[:, :BLOCK], n_v[b, i])

    def weights(b, i):
        for r in range(0, BLOCK, TILE):
            rows = pl.ds(i * BLOCK + r, TILE)
            d = decay_v[b, rows, :]
            c = c_v[b, rows, :]
            a = jnp.exp2(c)
            e = jnp.exp2(d * -unit - c)
            step = jnp.exp2(d * unit)
            a_out[b, rows, :] = a
            e_out[b, rows, :] = e
            x = drive_v[b, rows, :].astype(jnp.float32)
            grown = x * step
            v_v[b, rows, :] = (e * grown - x).astype(jnp.bfloat16)
            w_v[b, rows, :] = (a * grown - x).astype(jnp.bfloat16)

    def sums(b, i):
        rows = pl.ds(i * BLOCK, BLOCK)
        x = drive_v[b, rows, :]
        w = w_v[b, rows, :]
        f = dot(upto, stacked(x, v_v[b, rows, :]))
        q = dot(before, stacked(x, w))
        f_out[b, rows, :] = f
        q_out[b, rows, :] = q
        ends[1, b, pl.ds(i, 1), :] = f[last]
        ends[2, b, pl.ds(i, 1), :] = (
            q[last] + x[last].astype(jnp.float32) + w[last].astype(jnp.float32))

    for s in range(blocks + 3):
        if s in waits:
            for which in range(2):
                copy(which, s).wait()
        for b in range(batch):
            if s >= 3:
                sums(b, s - 3)
            if 1 <= s <= blocks:
                prefix(b, s - 1)
        for b in range(batch):
            if 2 <= s <= blocks + 1:
                weights(b, s - 2)
            if s < blocks:
                split(b, s)
    half = chans // 2
    for b in range(batch):
        fwd = bwd = jnp.zeros((1, chans), jnp.float32)
        p = jnp.ones((1, chans), jnp.float32)
        for i in range(blocks):
            j = blocks - 1 - i
            fwd = ends[0, b, i:i + 1, :] * (fwd + ends[1, b, i:i + 1, :])
            bwd = ends[2, b, j:j + 1, :] + ends[0, b, j:j + 1, :] * bwd
            p = p * ends[0, b, i:i + 1, :]
        for k in range(2):
            cols = slice(k * half, (k + 1) * half)
            r = 2 * b + k
            for side, val in ((0, fwd), (1, bwd)):
                tile[side, r:r + 1, :] = p[:, cols]
                tile[side, 4 + r:5 + r, :] = val[:, cols]
    rightward, leftward = tile[0], tile[1]
    for k in range(send.shape[0]):
        send[k] = jnp.where(k > me, rightward, leftward)


def states_kernel(recv, ends, a, e, f, q, gate, gated, power):
    batch, length, chans = a.shape
    blocks = length // BLOCK
    devices = recv.shape[0]
    me = lax.axis_index("time")
    fwd = jnp.zeros(recv.shape[1:], jnp.float32)
    bwd = fwd
    for j in range(devices):
        got = recv[j]
        fwd = (jnp.where(j < me, pltpu.roll(got, 4, 0), 1.0) * fwd
               + jnp.where(j < me, got, 0.0))
        j = devices - 1 - j
        got = recv[j]
        bwd = (jnp.where(j > me, pltpu.roll(got, 4, 0), 1.0) * bwd
               + jnp.where(j > me, got, 0.0))
    half = chans // 2
    for b in range(batch):
        alpha = [[None] * blocks for _ in range(2)]
        beta = [[None] * blocks for _ in range(2)]
        for k in range(2):
            cols = pl.ds(k * half, half)
            r = 4 + 2 * b + k
            state = fwd[r:r + 1]
            for i in range(blocks):
                alpha[k][i] = state
                state = ends[0, b, i:i + 1, cols] * (state + ends[1, b, i:i + 1, cols])
            state = bwd[r:r + 1]
            for i in reversed(range(blocks)):
                state = ends[2, b, i:i + 1, cols] + ends[0, b, i:i + 1, cols] * state
                beta[k][i] = state
        for i in range(blocks):
            rows = pl.ds(i * BLOCK, BLOCK)
            total = None
            for k in range(2):
                cols = pl.ds(k * half, half)
                h = gate[b, rows, cols].astype(jnp.float32) * 0.5
                s = (h + h * jnp.tanh(h)) * (
                    a[b, rows, cols] * (f[b, rows, cols] + alpha[k][i])
                    + e[b, rows, cols] * (beta[k][i] - q[b, rows, cols]))
                gated[b, rows, cols] = s
                total = s * s if k == 0 else total + s * s
            power[b, i:i + 1, :] = jnp.sum(total.T, axis=0, keepdims=True)


def scale_kernel(count, scale, gated, own, p1, p2, p3, gain, out, stage, sems):
    batch, length, chans = gated.shape
    blocks = length // BLOCK
    half = chans // 2
    total = own[...] + p1[...] + p2[...] + p3[...]
    r = lax.rsqrt(total * (scale * scale / count) + 1e-06) * scale
    copies = []
    for start, stop in zip(OUT, OUT[1:] + (blocks,)):
        for i in range(start, stop):
            rows = pl.ds(i * BLOCK, BLOCK)
            for b in range(batch):
                m = jnp.broadcast_to(r[b, i:i + 1, :], (BLOCK, BLOCK)).T
                for k in range(2):
                    cols = pl.ds(k * half, half)
                    stage[b, rows, cols] = (
                        gated[b, rows, cols] * m * gain[:, cols]
                    ).astype(jnp.bfloat16)
        rows = pl.ds(start * BLOCK, (stop - start) * BLOCK)
        copies.append(pltpu.make_async_copy(
            stage.at[:, rows, :], out.at[:, rows, :], sems.at[len(copies)]))
        copies[-1].start()
    for c in copies:
        c.wait()


def on_device(decay_rate, drive_in, gate_in, norm_gain):
    batch, length, chans = decay_rate.shape
    blocks = length // BLOCK
    devices = lax.axis_size("time")
    chan_devices = lax.axis_size("chan")
    total_length = length * devices
    f32 = jnp.float32
    vmem = pl.BlockSpec(memory_space=pltpu.VMEM)
    hbm = pl.BlockSpec(memory_space=pltpu.HBM)
    full = jax.ShapeDtypeStruct((batch, length, chans), f32)
    a, e, f, q, ends, send = pl.pallas_call(
        functools.partial(local_kernel, total_length),
        out_shape=(full,) * 4 + (
            jax.ShapeDtypeStruct((3, batch, blocks, chans), f32),
            jax.ShapeDtypeStruct((devices, 8, 128), f32)),
        in_specs=[hbm] * 2,
        out_specs=(vmem,) * 6,
        scratch_shapes=[
            pltpu.VMEM((batch, length, chans), f32),
            pltpu.VMEM((batch, length, chans), jnp.bfloat16),
            pltpu.VMEM((batch, blocks, BLOCK, chans), jnp.bfloat16),
            pltpu.VMEM((batch, length, chans), f32),
            pltpu.VMEM((batch, length, chans), jnp.bfloat16),
            pltpu.VMEM((batch, length, chans), jnp.bfloat16),
            pltpu.VMEM((2, 8, 128), f32),
            pltpu.SemaphoreType.DMA((2, blocks)),
        ],
        compiler_params=pltpu.CompilerParams(vmem_limit_bytes=32 << 20),
        name="local",
    )(*(pltpu.with_memory_space_constraint(t, pltpu.HBM)
        for t in (decay_rate, drive_in)))
    recv = lax.all_to_all(send, "time", 0, 0)
    gated, power = pl.pallas_call(
        states_kernel,
        out_shape=(full, jax.ShapeDtypeStruct((batch, blocks, BLOCK), f32)),
        in_specs=[vmem] * 7,
        out_specs=(vmem,) * 2,
        compiler_params=pltpu.CompilerParams(vmem_limit_bytes=32 << 20),
        name="states",
    )(recv, ends, a, e, f, q, gate_in)
    others = [
        lax.ppermute(power, "chan", [(i, i ^ k) for i in range(chan_devices)])
        for k in range(1, chan_devices)
    ]
    return pl.pallas_call(
        functools.partial(scale_kernel, chans * chan_devices, float(total_length) ** -0.5),
        out_shape=jax.ShapeDtypeStruct((batch, length, chans), jnp.bfloat16),
        in_specs=[vmem] * 6,
        out_specs=hbm,
        scratch_shapes=[
            pltpu.VMEM((batch, length, chans), jnp.bfloat16),
            pltpu.SemaphoreType.DMA((blocks,)),
        ],
        compiler_params=pltpu.CompilerParams(vmem_limit_bytes=32 << 20),
        name="scale",
    )(gated, power, *others, norm_gain.reshape(1, chans))


def solution(mesh):
    spec = P("ens", "time", "chan")
    return jax.shard_map(
        on_device, mesh=mesh, in_specs=(spec, spec, spec, P(("ens", "chan"))),
        out_specs=spec, check_vma=False,
    )
```

```python
import functools

import jax
import jax.numpy as jnp
from jax import lax
from jax.experimental import pallas as pl
from jax.experimental.pallas import tpu as pltpu
from jax.sharding import PartitionSpec as P

BLOCK = 128
TILE = 16
WAITS = (0, 1, 3, 5)
LATE = 0
OUT = (0, 1, 2, 3, 4, 5, 6, 7)
LOG2E = 1.4426950408889634


def triangle(strict):
    row = lax.broadcasted_iota(jnp.int32, (BLOCK, 2 * BLOCK), 0)
    col = lax.broadcasted_iota(jnp.int32, (BLOCK, 2 * BLOCK), 1)
    col = jnp.where(col >= BLOCK, col - BLOCK, col)
    keep = col < row if strict else col <= row
    return jnp.where(keep, 1.0, 0.0).astype(jnp.bfloat16)


def stacked(top, bottom):
    return jnp.concatenate([top, bottom], axis=0)


def local_kernel(total_length, decay, drive, gate, a_out, e_out, f_out, q_out, ends, send, gate_out,
                 decay_v, drive_v, n_v, c_v, v_v, w_v, tile, sems, gate_sem):
    batch, length, chans = decay.shape
    blocks = length // BLOCK
    me = lax.axis_index("time")
    unit = LOG2E / total_length
    pairs = ((decay, decay_v), (drive, drive_v))

    waits = {at: stop for at, stop in zip(WAITS, WAITS[1:] + (blocks,))}

    def copy(which, i):
        src, dst = pairs[which]
        rows = pl.ds(i * BLOCK, (waits[i] - i) * BLOCK)
        return pltpu.make_async_copy(
            src.at[:, rows, :], dst.at[:, rows, :], sems.at[which, i])

    for i in WAITS:
        for which in range(2):
            copy(which, i).start()
    upto = triangle(False)
    before = triangle(True)
    dot = functools.partial(jnp.dot, preferred_element_type=jnp.float32)
    last = slice(BLOCK - 1, BLOCK)

    def split(b, i):
        for r in range(0, BLOCK, TILE):
            n = decay_v[b, pl.ds(i * BLOCK + r, TILE), :] * -unit
            n_v[b, i, pl.ds(r, TILE), :] = n.astype(jnp.bfloat16)
            part = n if r == 0 else part + n
        ends[0, b, pl.ds(i, 1), :] = jnp.exp2(jnp.sum(part, axis=0, keepdims=True))

    def prefix(b, i):
        c_v[b, pl.ds(i * BLOCK, BLOCK), :] = dot(upto[:, :BLOCK], n_v[b, i])

    def weights(b, i):
        for r in range(0, BLOCK, TILE):
            rows = pl.ds(i * BLOCK + r, TILE)
            d = decay_v[b, rows, :]
            c = c_v[b, rows, :]
            a = jnp.exp2(c)
            e = jnp.exp2(d * -unit - c)
            step = jnp.exp2(d * unit)
            a_out[b, rows, :] = a
            e_out[b, rows, :] = e
            x = drive_v[b, rows, :].astype(jnp.float32)
            grown = x * step
            v_v[b, rows, :] = (e * grown - x).astype(jnp.bfloat16)
            w_v[b, rows, :] = (a * grown - x).astype(jnp.bfloat16)

    def sums(b, i):
        rows = pl.ds(i * BLOCK, BLOCK)
        x = drive_v[b, rows, :]
        w = w_v[b, rows, :]
        f = dot(upto, stacked(x, v_v[b, rows, :]))
        q = dot(before, stacked(x, w))
        f_out[b, rows, :] = f
        q_out[b, rows, :] = q
        ends[1, b, pl.ds(i, 1), :] = f[last]
        ends[2, b, pl.ds(i, 1), :] = (
            q[last] + x[last].astype(jnp.float32) + w[last].astype(jnp.float32))

    for s in range(blocks + 3):
        if s in waits:
            for which in range(2):
                copy(which, s).wait()
            if s == WAITS[LATE]:
                gate_copy = pltpu.make_async_copy(gate, gate_out, gate_sem)
                gate_copy.start()
        for b in range(batch):
            if s >= 3:
                sums(b, s - 3)
            if 1 <= s <= blocks:
                prefix(b, s - 1)
        for b in range(batch):
            if 2 <= s <= blocks + 1:
                weights(b, s - 2)
            if s < blocks:
                split(b, s)
    half = chans // 2
    for b in range(batch):
        fwd = bwd = jnp.zeros((1, chans), jnp.float32)
        p = jnp.ones((1, chans), jnp.float32)
        for i in range(blocks):
            j = blocks - 1 - i
            fwd = ends[0, b, i:i + 1, :] * (fwd + ends[1, b, i:i + 1, :])
            bwd = ends[2, b, j:j + 1, :] + ends[0, b, j:j + 1, :] * bwd
            p = p * ends[0, b, i:i + 1, :]
        for k in range(2):
            cols = slice(k * half, (k + 1) * half)
            r = 2 * b + k
            for side, val in ((0, fwd), (1, bwd)):
                tile[side, r:r + 1, :] = p[:, cols]
                tile[side, 4 + r:5 + r, :] = val[:, cols]
    rightward, leftward = tile[0], tile[1]
    for k in range(send.shape[0]):
        send[k] = jnp.where(k > me, rightward, leftward)
    gate_copy.wait()


def states_kernel(recv, ends, a, e, f, q, gate, gated, power):
    batch, length, chans = a.shape
    blocks = length // BLOCK
    devices = recv.shape[0]
    me = lax.axis_index("time")
    fwd = jnp.zeros(recv.shape[1:], jnp.float32)
    bwd = fwd
    for j in range(devices):
        got = recv[j]
        fwd = (jnp.where(j < me, pltpu.roll(got, 4, 0), 1.0) * fwd
               + jnp.where(j < me, got, 0.0))
        j = devices - 1 - j
        got = recv[j]
        bwd = (jnp.where(j > me, pltpu.roll(got, 4, 0), 1.0) * bwd
               + jnp.where(j > me, got, 0.0))
    half = chans // 2
    for b in range(batch):
        alpha = [[None] * blocks for _ in range(2)]
        beta = [[None] * blocks for _ in range(2)]
        for k in range(2):
            cols = pl.ds(k * half, half)
            r = 4 + 2 * b + k
            state = fwd[r:r + 1]
            for i in range(blocks):
                alpha[k][i] = state
                state = ends[0, b, i:i + 1, cols] * (state + ends[1, b, i:i + 1, cols])
            state = bwd[r:r + 1]
            for i in reversed(range(blocks)):
                state = ends[2, b, i:i + 1, cols] + ends[0, b, i:i + 1, cols] * state
                beta[k][i] = state
        for i in range(blocks):
            rows = pl.ds(i * BLOCK, BLOCK)
            total = None
            for k in range(2):
                cols = pl.ds(k * half, half)
                h = gate[b, rows, cols].astype(jnp.float32)
                s = h * lax.logistic(h) * (
                    a[b, rows, cols] * (f[b, rows, cols] + alpha[k][i])
                    + e[b, rows, cols] * (beta[k][i] - q[b, rows, cols]))
                gated[b, rows, cols] = s
                total = s * s if k == 0 else total + s * s
            power[b, i:i + 1, :] = jnp.sum(total.T, axis=0, keepdims=True)


def scale_kernel(count, scale, gated, own, p1, p2, p3, gain, out, stage, sems):
    batch, length, chans = gated.shape
    blocks = length // BLOCK
    half = chans // 2
    total = own[...] + p1[...] + p2[...] + p3[...]
    r = lax.rsqrt(total * (scale * scale / count) + 1e-06) * scale
    copies = []
    for start, stop in zip(OUT, OUT[1:] + (blocks,)):
        for i in range(start, stop):
            rows = pl.ds(i * BLOCK, BLOCK)
            for b in range(batch):
                m = jnp.broadcast_to(r[b, i:i + 1, :], (BLOCK, BLOCK)).T
                for k in range(2):
                    cols = pl.ds(k * half, half)
                    stage[b, rows, cols] = (
                        gated[b, rows, cols] * m * gain[:, cols]
                    ).astype(jnp.bfloat16)
        rows = pl.ds(start * BLOCK, (stop - start) * BLOCK)
        copies.append(pltpu.make_async_copy(
            stage.at[:, rows, :], out.at[:, rows, :], sems.at[len(copies)]))
        copies[-1].start()
    for c in copies:
        c.wait()


def on_device(decay_rate, drive_in, gate_in, norm_gain):
    batch, length, chans = decay_rate.shape
    blocks = length // BLOCK
    devices = lax.axis_size("time")
    chan_devices = lax.axis_size("chan")
    total_length = length * devices
    f32 = jnp.float32
    vmem = pl.BlockSpec(memory_space=pltpu.VMEM)
    hbm = pl.BlockSpec(memory_space=pltpu.HBM)
    full = jax.ShapeDtypeStruct((batch, length, chans), f32)
    a, e, f, q, ends, send, gate = pl.pallas_call(
        functools.partial(local_kernel, total_length),
        out_shape=(full,) * 4 + (
            jax.ShapeDtypeStruct((3, batch, blocks, chans), f32),
            jax.ShapeDtypeStruct((devices, 8, 128), f32),
            jax.ShapeDtypeStruct((batch, length, chans), jnp.bfloat16)),
        in_specs=[hbm] * 3,
        out_specs=(vmem,) * 7,
        scratch_shapes=[
            pltpu.VMEM((batch, length, chans), f32),
            pltpu.VMEM((batch, length, chans), jnp.bfloat16),
            pltpu.VMEM((batch, blocks, BLOCK, chans), jnp.bfloat16),
            pltpu.VMEM((batch, length, chans), f32),
            pltpu.VMEM((batch, length, chans), jnp.bfloat16),
            pltpu.VMEM((batch, length, chans), jnp.bfloat16),
            pltpu.VMEM((2, 8, 128), f32),
            pltpu.SemaphoreType.DMA((2, blocks)),
            pltpu.SemaphoreType.DMA,
        ],
        compiler_params=pltpu.CompilerParams(vmem_limit_bytes=32 << 20),
        name="local",
    )(*(pltpu.with_memory_space_constraint(t, pltpu.HBM)
        for t in (decay_rate, drive_in, gate_in)))
    recv = lax.all_to_all(send, "time", 0, 0)
    gated, power = pl.pallas_call(
        states_kernel,
        out_shape=(full, jax.ShapeDtypeStruct((batch, blocks, BLOCK), f32)),
        in_specs=[vmem] * 7,
        out_specs=(vmem,) * 2,
        compiler_params=pltpu.CompilerParams(vmem_limit_bytes=32 << 20),
        name="states",
    )(recv, ends, a, e, f, q, gate)
    others = [
        lax.ppermute(power, "chan", [(i, i ^ k) for i in range(chan_devices)])
        for k in range(1, chan_devices)
    ]
    return pl.pallas_call(
        functools.partial(scale_kernel, chans * chan_devices, float(total_length) ** -0.5),
        out_shape=jax.ShapeDtypeStruct((batch, length, chans), jnp.bfloat16),
        in_specs=[vmem] * 6,
        out_specs=hbm,
        scratch_shapes=[
            pltpu.VMEM((batch, length, chans), jnp.bfloat16),
            pltpu.SemaphoreType.DMA((blocks,)),
        ],
        compiler_params=pltpu.CompilerParams(vmem_limit_bytes=32 << 20),
        name="scale",
    )(gated, power, *others, norm_gain.reshape(1, chans))


def solution(mesh):
    spec = P("ens", "time", "chan")
    return jax.shard_map(
        on_device, mesh=mesh, in_specs=(spec, spec, spec, P(("ens", "chan"))),
        out_specs=spec, check_vma=False,
    )
```

```python
import functools

import jax
import jax.numpy as jnp
from jax import lax
from jax.experimental import pallas as pl
from jax.experimental.pallas import tpu as pltpu
from jax.sharding import PartitionSpec as P

BLOCK = 128
TILE = 16
WAITS = (0, 1, 3, 5)
LATE = 0
OUT = (0, 1, 2, 3, 4, 5, 6, 7)
LOG2E = 1.4426950408889634


def triangle(strict):
    row = lax.broadcasted_iota(jnp.int32, (BLOCK, 2 * BLOCK), 0)
    col = lax.broadcasted_iota(jnp.int32, (BLOCK, 2 * BLOCK), 1)
    col = jnp.where(col >= BLOCK, col - BLOCK, col)
    keep = col < row if strict else col <= row
    return jnp.where(keep, 1.0, 0.0).astype(jnp.bfloat16)


def stacked(top, bottom):
    return jnp.concatenate([top, bottom], axis=0)


def local_kernel(total_length, decay, drive, gate, a_out, e_out, f_out, q_out, ends, send, gate_out,
                 decay_v, drive_v, n_v, c_v, v_v, w_v, tile, sems, gate_sem):
    batch, length, chans = decay.shape
    blocks = length // BLOCK
    me = lax.axis_index("time")
    unit = LOG2E / total_length
    pairs = ((decay, decay_v), (drive, drive_v))

    waits = {at: stop for at, stop in zip(WAITS, WAITS[1:] + (blocks,))}

    def copy(which, i):
        src, dst = pairs[which]
        rows = pl.ds(i * BLOCK, (waits[i] - i) * BLOCK)
        return pltpu.make_async_copy(
            src.at[:, rows, :], dst.at[:, rows, :], sems.at[which, i])

    for i in WAITS:
        for which in range(2):
            copy(which, i).start()
    upto = triangle(False)
    before = triangle(True)
    dot = functools.partial(jnp.dot, preferred_element_type=jnp.float32)
    last = slice(BLOCK - 1, BLOCK)

    def split(b, i):
        for r in range(0, BLOCK, TILE):
            n = decay_v[b, pl.ds(i * BLOCK + r, TILE), :] * -unit
            n_v[b, i, pl.ds(r, TILE), :] = n.astype(jnp.bfloat16)
            part = n if r == 0 else part + n
        ends[0, b, pl.ds(i, 1), :] = jnp.exp2(jnp.sum(part, axis=0, keepdims=True))

    def prefix(b, i):
        c_v[b, pl.ds(i * BLOCK, BLOCK), :] = dot(upto[:, :BLOCK], n_v[b, i])

    def weights(b, i):
        for r in range(0, BLOCK, TILE):
            rows = pl.ds(i * BLOCK + r, TILE)
            d = decay_v[b, rows, :]
            c = c_v[b, rows, :]
            a = jnp.exp2(c)
            e = jnp.exp2(d * -unit - c)
            step = jnp.exp2(d * unit)
            a_out[b, rows, :] = a
            e_out[b, rows, :] = e
            x = drive_v[b, rows, :].astype(jnp.float32)
            grown = x * step
            v_v[b, rows, :] = (e * grown - x).astype(jnp.bfloat16)
            w_v[b, rows, :] = (a * grown - x).astype(jnp.bfloat16)

    def sums(b, i):
        rows = pl.ds(i * BLOCK, BLOCK)
        x = drive_v[b, rows, :]
        w = w_v[b, rows, :]
        f = dot(upto, stacked(x, v_v[b, rows, :]))
        q = dot(before, stacked(x, w))
        f_out[b, rows, :] = f
        q_out[b, rows, :] = q
        ends[1, b, pl.ds(i, 1), :] = f[last]
        ends[2, b, pl.ds(i, 1), :] = (
            q[last] + x[last].astype(jnp.float32) + w[last].astype(jnp.float32))

    for s in range(blocks + 3):
        if s in waits:
            for which in range(2):
                copy(which, s).wait()
            if s == WAITS[LATE]:
                gate_copy = pltpu.make_async_copy(gate, gate_out, gate_sem)
                gate_copy.start()
        for b in range(batch):
            if s >= 3:
                sums(b, s - 3)
            if 1 <= s <= blocks:
                prefix(b, s - 1)
        for b in range(batch):
            if 2 <= s <= blocks + 1:
                weights(b, s - 2)
            if s < blocks:
                split(b, s)
    half = chans // 2
    for b in range(batch):
        fwd = bwd = jnp.zeros((1, chans), jnp.float32)
        p = jnp.ones((1, chans), jnp.float32)
        for i in range(blocks):
            j = blocks - 1 - i
            fwd = ends[0, b, i:i + 1, :] * (fwd + ends[1, b, i:i + 1, :])
            bwd = ends[2, b, j:j + 1, :] + ends[0, b, j:j + 1, :] * bwd
            p = p * ends[0, b, i:i + 1, :]
        for k in range(2):
            cols = slice(k * half, (k + 1) * half)
            r = 2 * b + k
            for side, val in ((0, fwd), (1, bwd)):
                tile[side, r:r + 1, :] = p[:, cols]
                tile[side, 4 + r:5 + r, :] = val[:, cols]
    rightward, leftward = tile[0], tile[1]
    for k in range(send.shape[0]):
        send[k] = jnp.where(k > me, rightward, leftward)
    gate_copy.wait()


def states_kernel(recv, ends, a, e, f, q, gate, gated, power):
    batch, length, chans = a.shape
    blocks = length // BLOCK
    devices = recv.shape[0]
    me = lax.axis_index("time")
    fwd = jnp.zeros(recv.shape[1:], jnp.float32)
    bwd = fwd
    for j in range(devices):
        got = recv[j]
        fwd = (jnp.where(j < me, pltpu.roll(got, 4, 0), 1.0) * fwd
               + jnp.where(j < me, got, 0.0))
        j = devices - 1 - j
        got = recv[j]
        bwd = (jnp.where(j > me, pltpu.roll(got, 4, 0), 1.0) * bwd
               + jnp.where(j > me, got, 0.0))
    half = chans // 2
    for b in range(batch):
        alpha = [[None] * blocks for _ in range(2)]
        beta = [[None] * blocks for _ in range(2)]
        for k in range(2):
            cols = pl.ds(k * half, half)
            r = 4 + 2 * b + k
            state = fwd[r:r + 1]
            for i in range(blocks):
                alpha[k][i] = state
                state = ends[0, b, i:i + 1, cols] * (state + ends[1, b, i:i + 1, cols])
            state = bwd[r:r + 1]
            for i in reversed(range(blocks)):
                state = ends[2, b, i:i + 1, cols] + ends[0, b, i:i + 1, cols] * state
                beta[k][i] = state
        for i in range(blocks):
            rows = pl.ds(i * BLOCK, BLOCK)
            total = None
            for k in range(2):
                cols = pl.ds(k * half, half)
                h = gate[b, rows, cols].astype(jnp.float32)
                s = h * lax.logistic(h) * (
                    a[b, rows, cols] * (f[b, rows, cols] + alpha[k][i])
                    + e[b, rows, cols] * (beta[k][i] - q[b, rows, cols]))
                gated[b, rows, cols] = s
                total = s * s if k == 0 else total + s * s
            power[b, i:i + 1, :] = jnp.sum(total.T, axis=0, keepdims=True)


def scale_kernel(count, scale, gated, own, p1, p2, p3, gain, out, stage, sems):
    batch, length, chans = gated.shape
    blocks = length // BLOCK
    half = chans // 2
    total = own[...] + p1[...] + p2[...] + p3[...]
    r = lax.rsqrt(total * (scale * scale / count) + 1e-06) * scale
    copies = []
    for start, stop in zip(OUT, OUT[1:] + (blocks,)):
        for i in range(start, stop):
            rows = pl.ds(i * BLOCK, BLOCK)
            for b in range(batch):
                m = jnp.broadcast_to(r[b, i:i + 1, :], (BLOCK, BLOCK)).T
                for k in range(2):
                    cols = pl.ds(k * half, half)
                    stage[b, rows, cols] = (
                        gated[b, rows, cols] * m * gain[:, cols]
                    ).astype(jnp.bfloat16)
        rows = pl.ds(start * BLOCK, (stop - start) * BLOCK)
        copies.append(pltpu.make_async_copy(
            stage.at[:, rows, :], out.at[:, rows, :], sems.at[len(copies)]))
        copies[-1].start()
    for c in copies:
        c.wait()


def on_device(decay_rate, drive_in, gate_in, norm_gain):
    batch, length, chans = decay_rate.shape
    blocks = length // BLOCK
    devices = lax.axis_size("time")
    chan_devices = lax.axis_size("chan")
    total_length = length * devices
    f32 = jnp.float32
    vmem = pl.BlockSpec(memory_space=pltpu.VMEM)
    hbm = pl.BlockSpec(memory_space=pltpu.HBM)
    full = jax.ShapeDtypeStruct((batch, length, chans), f32)
    a, e, f, q, ends, send, gate = pl.pallas_call(
        functools.partial(local_kernel, total_length),
        out_shape=(full,) * 4 + (
            jax.ShapeDtypeStruct((3, batch, blocks, chans), f32),
            jax.ShapeDtypeStruct((devices, 8, 128), f32),
            jax.ShapeDtypeStruct((batch, length, chans), jnp.bfloat16)),
        in_specs=[hbm] * 3,
        out_specs=(vmem,) * 7,
        scratch_shapes=[
            pltpu.VMEM((batch, length, chans), f32),
            pltpu.VMEM((batch, length, chans), jnp.bfloat16),
            pltpu.VMEM((batch, blocks, BLOCK, chans), jnp.bfloat16),
            pltpu.VMEM((batch, length, chans), f32),
            pltpu.VMEM((batch, length, chans), jnp.bfloat16),
            pltpu.VMEM((batch, length, chans), jnp.bfloat16),
            pltpu.VMEM((2, 8, 128), f32),
            pltpu.SemaphoreType.DMA((2, blocks)),
            pltpu.SemaphoreType.DMA,
        ],
        compiler_params=pltpu.CompilerParams(vmem_limit_bytes=32 << 20),
        name="local",
    )(*(pltpu.with_memory_space_constraint(t, pltpu.HBM)
        for t in (decay_rate, drive_in, gate_in)))
    recv = lax.all_to_all(send, "time", 0, 0)
    gated, power = pl.pallas_call(
        states_kernel,
        out_shape=(full, jax.ShapeDtypeStruct((batch, blocks, BLOCK), f32)),
        in_specs=[vmem] * 7,
        out_specs=(vmem,) * 2,
        compiler_params=pltpu.CompilerParams(vmem_limit_bytes=32 << 20),
        name="states",
    )(recv, ends, a, e, f, q, gate)
    others = [
        lax.ppermute(power, "chan", [(i, i ^ k) for i in range(chan_devices)])
        for k in (1, 3, 2)
    ]
    return pl.pallas_call(
        functools.partial(scale_kernel, chans * chan_devices, float(total_length) ** -0.5),
        out_shape=jax.ShapeDtypeStruct((batch, length, chans), jnp.bfloat16),
        in_specs=[vmem] * 6,
        out_specs=hbm,
        scratch_shapes=[
            pltpu.VMEM((batch, length, chans), jnp.bfloat16),
            pltpu.SemaphoreType.DMA((blocks,)),
        ],
        compiler_params=pltpu.CompilerParams(vmem_limit_bytes=32 << 20),
        name="scale",
    )(gated, power, *others, norm_gain.reshape(1, chans))


def solution(mesh):
    spec = P("ens", "time", "chan")
    return jax.shard_map(
        on_device, mesh=mesh, in_specs=(spec, spec, spec, P(("ens", "chan"))),
        out_specs=spec, check_vma=False,
    )
```
